16 devices in a mesh: tp: 2 (over z), fsdp: 8 (over y, x, core).
Axes of the slice: x: 2, y: 2, z: 2, core: 2. Of those that a mesh axis runs over, the one named last changes fastest.
Arguments:
- x_in: bfloat16 [24, 1024, 2048], P('fsdp')
- dy_out: bfloat16 [24, 1024, 2048], P('fsdp')
- ln_gain: float32 [2048], P('fsdp')
- w_q: bfloat16 [2048, 2048], P('fsdp', 'tp')
- w_k: bfloat16 [2048, 128], P('fsdp')
- w_v: bfloat16 [2048, 128], P('fsdp')
- w_o: bfloat16 [2048, 2048], P('tp', 'fsdp')
- w_gate: bfloat16 [2048, 8192], P('fsdp', 'tp')
- w_up: bfloat16 [2048, 8192], P('fsdp', 'tp')
- w_down: bfloat16 [8192, 2048], P('tp', 'fsdp')
Outputs:
- output 1: bfloat16 [24, 1024, 2048], P('fsdp')
- output 2: bfloat16 [24, 1024, 2048], P('fsdp')
- output 3: float32 [2048], P('fsdp')
- output 4: float32 [2048, 2048], P('fsdp', 'tp')
- output 5: float32 [2048, 128], P('fsdp')
- output 6: float32 [2048, 128], P('fsdp')
- output 7: float32 [2048, 2048], P('tp', 'fsdp')
- output 8: float32 [2048, 8192], P('fsdp', 'tp')
- output 9: float32 [2048, 8192], P('fsdp', 'tp')
- output 10: float32 [8192, 2048], P('tp', 'fsdp')
All inputs are finite; a program needn't handle non-finite values.
Results may differ from the reference program's by a relative error of at most 0.0155669.
Values are sent between devices in bfloat16 or wider.
A program may use at most 1 GiB of HBM per device.

```python
import math
import jax
import jax.numpy as jnp
from jax import lax

D_MODEL = 2048
N_HEADS = 16
HEAD_DIM = 128
D_FF = 8192
N_BATCH = 24
SEQ_LEN = 1024


def setup_inputs(seed: int = 0) -> dict:
    keys = jax.random.split(jax.random.key(seed), 10)
    inner = N_HEADS * HEAD_DIM
    scale_model = 1.0 / math.sqrt(D_MODEL)

    def draw_normal(slot, shape, scale):
        return (jax.random.normal(keys[slot], shape, jnp.float32) * scale).astype(jnp.bfloat16)

    return {
        'x_in': draw_normal(0, (N_BATCH, SEQ_LEN, D_MODEL), 1.0),
        'dy_out': draw_normal(1, (N_BATCH, SEQ_LEN, D_MODEL), 1.0),
        'ln_gain': jax.random.uniform(keys[2], (D_MODEL,), jnp.float32, 0.5, 1.5),
        'w_q': draw_normal(3, (D_MODEL, inner), scale_model),
        'w_k': draw_normal(4, (D_MODEL, HEAD_DIM), scale_model),
        'w_v': draw_normal(5, (D_MODEL, HEAD_DIM), scale_model),
        'w_o': draw_normal(6, (inner, D_MODEL), 1.0 / math.sqrt(inner)),
        'w_gate': draw_normal(7, (D_MODEL, D_FF), scale_model),
        'w_up': draw_normal(8, (D_MODEL, D_FF), scale_model),
        'w_down': draw_normal(9, (D_FF, D_MODEL), 1.0 / math.sqrt(D_FF)),
    }


def to_bf16(vals):
    return vals.astype(jnp.bfloat16).astype(jnp.float32)


def layer_norm(x_f32, gain):
    x_mean = jnp.mean(x_f32, axis=-1, keepdims=True)
    x_cent = x_f32 - x_mean
    x_var = jnp.mean(x_cent * x_cent, axis=-1, keepdims=True)
    return to_bf16(x_cent * lax.rsqrt(x_var + 1e-5) * gain)


def rope_tables():
    half_dim = HEAD_DIM // 2
    inv_freq = jnp.power(10000.0, -2.0 * jnp.arange(half_dim, dtype=jnp.float32) / HEAD_DIM)
    angle = jnp.arange(SEQ_LEN, dtype=jnp.float32)[:, None] * inv_freq[None, :]
    return jnp.cos(angle), jnp.sin(angle)


def rotate(vals, cos_t, sin_t):
    half_dim = vals.shape[-1] // 2
    first = vals[..., :half_dim]
    second = vals[..., half_dim:]
    return jnp.concatenate([first * cos_t - second * sin_t, second * cos_t + first * sin_t], axis=-1)


def attend_rows(q_rot, k_rot, v_val):
    causal = lax.broadcasted_iota(jnp.int32, (SEQ_LEN, SEQ_LEN), 0) >= lax.broadcasted_iota(jnp.int32, (SEQ_LEN, SEQ_LEN), 1)

    def one_head(q_head, k_row, v_row):
        scores = jnp.dot(q_head, k_row.T, preferred_element_type=jnp.float32)
        scores = jnp.where(causal, scores, -1e30)
        row_max = lax.stop_gradient(jnp.max(scores, axis=-1, keepdims=True))
        exp_val = jnp.exp(scores - row_max)
        att_prob = to_bf16(exp_val / jnp.sum(exp_val, axis=-1, keepdims=True))
        return to_bf16(jnp.dot(att_prob, v_row, preferred_element_type=jnp.float32))

    head_step = jax.checkpoint(one_head)

    def one_row(row):
        q_row, k_row, v_row = row

        def per_head(q_head):
            return head_step(q_head, k_row, v_row)

        head_outs = lax.map(per_head, jnp.swapaxes(q_row, 0, 1))
        return jnp.swapaxes(head_outs, 0, 1)

    return lax.map(one_row, (q_rot, k_rot, v_val))


def layer_forward(x_f32, gain, w_q, w_k, w_v, w_o, w_gate, w_up, w_down):
    n_batch = x_f32.shape[0]
    h_norm = layer_norm(x_f32, gain)
    q_raw = to_bf16(jnp.einsum('bsd,de->bse', h_norm, w_q))
    k_raw = to_bf16(jnp.einsum('bsd,de->bse', h_norm, w_k))
    v_val = to_bf16(jnp.einsum('bsd,de->bse', h_norm, w_v))
    gate_val = to_bf16(jnp.einsum('bsd,df->bsf', h_norm, w_gate))
    up_val = to_bf16(jnp.einsum('bsd,df->bsf', h_norm, w_up))
    cos_t, sin_t = rope_tables()
    q_heads = q_raw.reshape(n_batch, SEQ_LEN, N_HEADS, HEAD_DIM)
    q_rot = to_bf16(rotate(q_heads, cos_t[:, None, :], sin_t[:, None, :]) * (1.0 / math.sqrt(HEAD_DIM)))
    k_rot = to_bf16(rotate(k_raw, cos_t, sin_t))
    att_out = attend_rows(q_rot, k_rot, v_val).reshape(n_batch, SEQ_LEN, N_HEADS * HEAD_DIM)
    mlp_act = to_bf16(jax.nn.silu(gate_val) * up_val)
    branch = jnp.einsum('bse,ed->bsd', att_out, w_o) + jnp.einsum('bsf,fd->bsd', mlp_act, w_down)
    return x_f32 + branch


def reference(x_in, dy_out, ln_gain, w_q, w_k, w_v, w_o, w_gate, w_up, w_down):
    y_f32, pullback = jax.vjp(layer_forward, x_in.astype(jnp.float32), ln_gain, w_q.astype(jnp.float32), w_k.astype(jnp.float32), w_v.astype(jnp.float32), w_o.astype(jnp.float32), w_gate.astype(jnp.float32), w_up.astype(jnp.float32), w_down.astype(jnp.float32))
    gradients = pullback(dy_out.astype(jnp.float32))
    return (y_f32.astype(jnp.bfloat16), gradients[0].astype(jnp.bfloat16), gradients[1], gradients[2], gradients[3], gradients[4], gradients[5], gradients[6], gradients[7], gradients[8])
```

```python
import math
import jax
import jax.numpy as jnp
from jax import lax
from jax.experimental import pallas as pl
from jax.experimental.pallas import tpu as pltpu
from jax.sharding import PartitionSpec as P

F32 = jnp.float32
BF16 = jnp.bfloat16
HEAD = 128
ROWS = 256


def dot_f32(left, right, left_dim, right_dim):
    return lax.dot_general(left, right, (((left_dim,), (right_dim,)), ((), ())), preferred_element_type=F32)


def prep_kernel(me_ref, x_ref, dy_ref, gain_ref, h_ref, h_own_ref, h_peer_ref, dy_own_ref, dy_peer_ref):
    x = x_ref[...].astype(F32)
    x_cent = x - jnp.mean(x, axis=-1, keepdims=True)
    x_var = jnp.mean(x_cent * x_cent, axis=-1, keepdims=True)
    h_ref[...] = (x_cent * lax.rsqrt(x_var + 1e-5) * gain_ref[...]).astype(BF16)
    me = me_ref[0]
    width = h_own_ref.shape[1] // 4
    for slot in range(4):
        own = pl.ds(pl.multiple_of((me ^ (2 * slot)) * width, width), width)
        peer = pl.ds(pl.multiple_of((me ^ (2 * slot + 1)) * width, width), width)
        here = slice(slot * width, (slot + 1) * width)
        h_own_ref[:, here] = h_ref[:, own]
        h_peer_ref[:, here] = h_ref[:, peer]
        dy_own_ref[:, here] = dy_ref[:, own]
        dy_peer_ref[:, here] = dy_ref[:, peer]


def prep(me, x2, dy2, gain):
    n_tok, width = x2.shape
    full = pl.BlockSpec((ROWS, width), lambda i, s: (i, 0))
    half = pl.BlockSpec((ROWS, width // 2), lambda i, s: (i, 0))
    return pl.pallas_call(
        prep_kernel,
        grid_spec=pltpu.PrefetchScalarGridSpec(
            num_scalar_prefetch=1,
            grid=(n_tok // ROWS,),
            in_specs=[full, full, pl.BlockSpec((1, width), lambda i, s: (0, 0))],
            out_specs=[full, half, half, half, half],
        ),
        out_shape=[jax.ShapeDtypeStruct((n_tok, width), BF16)] + [jax.ShapeDtypeStruct((n_tok, width // 2), BF16)] * 4,
        cost_estimate=pl.CostEstimate(flops=20 * n_tok * width, bytes_accessed=10 * n_tok * width, transcendentals=0),
        name="prep",
    )(me, x2, dy2, gain)


def turn(vals, cos_t, sin_t):
    return vals * cos_t + pltpu.roll(vals, HEAD // 2, 1) * sin_t


def att_kernel(q_ref, k_ref, v_ref, do_ref, cos_ref, sin_ref, o_ref, dq_ref, dkv_ref):
    seq_len = q_ref.shape[0]
    scale = 1.0 / math.sqrt(HEAD)
    k = turn(k_ref[...].astype(F32), cos_ref[...], sin_ref[...]).astype(BF16)
    v = v_ref[...]

    @pl.when(pl.program_id(1) == 0)
    def _():
        dkv_ref[...] = jnp.zeros_like(dkv_ref)

    block = 256
    for i in range(seq_len // block):
        here = slice(i * block, (i + 1) * block)
        seen = (i + 1) * block
        cos_t = cos_ref[here, :]
        sin_t = sin_ref[here, :]
        q = (turn(q_ref[here, :].astype(F32), cos_t, sin_t) * scale).astype(BF16)
        d_out = do_ref[here, :]
        scores = dot_f32(q, k[:seen], 1, 1)
        row = lax.broadcasted_iota(jnp.int32, (block, seen), 0) + i * block
        col = lax.broadcasted_iota(jnp.int32, (block, seen), 1)
        scores = jnp.where(row >= col, scores, -1e30)
        exp_val = jnp.exp(scores - jnp.max(scores, axis=-1, keepdims=True))
        prob = exp_val * (1.0 / jnp.sum(exp_val, axis=-1, keepdims=True))
        prob_b = prob.astype(BF16)
        o_ref[here, :] = dot_f32(prob_b, v[:seen], 1, 0).astype(BF16)
        d_prob = dot_f32(d_out, v[:seen], 1, 1).astype(BF16).astype(F32)
        d_row = jnp.sum(d_prob * prob, axis=-1, keepdims=True)
        d_scores = (prob * (d_prob - d_row)).astype(BF16)
        d_q = dot_f32(d_scores, k[:seen], 1, 0).astype(BF16).astype(F32) * scale
        dq_ref[here, :] = turn(d_q, cos_t, -sin_t).astype(BF16)
        dkv_ref[:seen, :HEAD] += dot_f32(d_scores, q, 0, 0)
        dkv_ref[:seen, HEAD:] += dot_f32(prob_b, d_out, 0, 0)


def attention(qkv, d_att, cos_t, sin_t, seq_len):
    n_tok, inner = d_att.shape
    n_heads = inner // HEAD
    n_batch = n_tok // seq_len
    head = pl.BlockSpec((seq_len, HEAD), lambda b, h: (b, h))
    table = pl.BlockSpec((seq_len, HEAD), lambda b, h: (0, 0))
    flops = 12 * n_batch * n_heads * seq_len * seq_len * HEAD
    return pl.pallas_call(
        att_kernel,
        grid=(n_batch, n_heads),
        in_specs=[
            head,
            pl.BlockSpec((seq_len, HEAD), lambda b, h: (b, n_heads)),
            pl.BlockSpec((seq_len, HEAD), lambda b, h: (b, n_heads + 1)),
            head,
            table,
            table,
        ],
        out_specs=[head, head, pl.BlockSpec((seq_len, 2 * HEAD), lambda b, h: (b, 0))],
        out_shape=[
            jax.ShapeDtypeStruct((n_tok, inner), BF16),
            jax.ShapeDtypeStruct(qkv.shape, BF16),
            jax.ShapeDtypeStruct((n_tok, 2 * HEAD), F32),
        ],
        cost_estimate=pl.CostEstimate(flops=flops, bytes_accessed=8 * n_tok * inner, transcendentals=n_batch * n_heads * seq_len * seq_len),
        name="attention",
    )(qkv, qkv, qkv, d_att, cos_t, sin_t)


def kv_kernel(own_ref, peer_ref, cos_ref, sin_ref, held_ref, out_ref):
    total = (own_ref[...] + peer_ref[...]).astype(BF16)
    d_k = total[:, :HEAD].astype(F32)
    out_ref[:, :HEAD] = turn(d_k, cos_ref[...], -sin_ref[...]).astype(BF16)
    out_ref[:, HEAD:] = total[:, HEAD:]


def kv_finish(own, peer, cos_t, sin_t, d_qkv):
    n_tok = own.shape[0]
    per_seq = cos_t.shape[0] // ROWS
    part = pl.BlockSpec((ROWS, 2 * HEAD), lambda i: (i, 0))
    table = pl.BlockSpec((ROWS, HEAD), lambda i: (i % per_seq, 0))
    last = d_qkv.shape[1] // (2 * HEAD) - 1
    return pl.pallas_call(
        kv_kernel,
        grid=(n_tok // ROWS,),
        in_specs=[part, part, table, table, pl.BlockSpec(memory_space=pl.ANY)],
        out_specs=pl.BlockSpec((ROWS, 2 * HEAD), lambda i: (i, last)),
        out_shape=jax.ShapeDtypeStruct(d_qkv.shape, BF16),
        input_output_aliases={4: 0},
        cost_estimate=pl.CostEstimate(flops=20 * own.size, bytes_accessed=10 * own.size, transcendentals=0),
        name="kv_finish",
    )(own, peer, cos_t, sin_t, d_qkv)


def y_kernel(x_ref, own_ref, peer_ref, *refs):
    branch = own_ref[...].astype(F32) + peer_ref[...].astype(F32)
    refs[-1][...] = (x_ref[...].astype(F32) + branch).astype(BF16)


def y_finish(index, x2, own, peer, held):
    rows, width = own.shape
    steps = rows // ROWS
    whole = pl.BlockSpec((ROWS, width), lambda i: (index * steps + i, 0))
    part = pl.BlockSpec((ROWS, width), lambda i: (i, 0))
    extra = [] if held is None else [held]
    return pl.pallas_call(
        y_kernel,
        grid=(steps,),
        in_specs=[whole, part, part] + [pl.BlockSpec(memory_space=pl.ANY)] * len(extra),
        out_specs=whole,
        out_shape=jax.ShapeDtypeStruct(x2.shape, BF16),
        input_output_aliases={3: 0} if extra else {},
        cost_estimate=pl.CostEstimate(flops=20 * own.size, bytes_accessed=8 * own.size, transcendentals=0),
        name="y_finish",
    )(x2, own, peer, *extra)


def norm_kernel(x_ref, dy_ref, own_ref, peer_ref, gain_ref, *refs):
    grad_ref, part_ref = refs[-2:]

    @pl.when(pl.program_id(0) == 0)
    def _():
        part_ref[...] = jnp.zeros_like(part_ref)

    x = x_ref[...].astype(F32)
    x_cent = x - jnp.mean(x, axis=-1, keepdims=True)
    rstd = lax.rsqrt(jnp.mean(x_cent * x_cent, axis=-1, keepdims=True) + 1e-5)
    x_hat = x_cent * rstd
    d_h = (own_ref[...].astype(F32) + peer_ref[...].astype(F32)).astype(BF16).astype(F32)
    part_ref[...] += jnp.sum(d_h * x_hat, axis=0, keepdims=True)
    d_hat = d_h * gain_ref[...]
    mean_d = jnp.mean(d_hat, axis=-1, keepdims=True)
    mean_dx = jnp.mean(d_hat * x_hat, axis=-1, keepdims=True)
    d_x = rstd * (d_hat - mean_d - x_hat * mean_dx)
    grad_ref[...] = (dy_ref[...].astype(F32) + d_x).astype(BF16)


def norm_finish(index, x2, dy2, own, peer, gain, held):
    rows, width = own.shape
    steps = rows // ROWS
    whole = pl.BlockSpec((ROWS, width), lambda i: (index * steps + i, 0))
    part = pl.BlockSpec((ROWS, width), lambda i: (i, 0))
    line = pl.BlockSpec((1, width), lambda i: (0, 0))
    extra = [] if held is None else [held]
    return pl.pallas_call(
        norm_kernel,
        grid=(steps,),
        in_specs=[whole, whole, part, part, line] + [pl.BlockSpec(memory_space=pl.ANY)] * len(extra),
        out_specs=[whole, line],
        out_shape=[jax.ShapeDtypeStruct(x2.shape, BF16), jax.ShapeDtypeStruct((1, width), F32)],
        input_output_aliases={5: 0} if extra else {},
        cost_estimate=pl.CostEstimate(flops=50 * own.size, bytes_accessed=10 * own.size, transcendentals=0),
        name="norm_finish",
    )(x2, dy2, own, peer, gain, *extra)


def swiglu(gate_val, up_val):
    return (jax.nn.silu(gate_val.astype(F32)) * up_val.astype(F32)).astype(BF16)


def swap(vals, bit, n_dev):
    return lax.ppermute(vals, 'fsdp', [(i, i ^ bit) for i in range(n_dev)])


def after(vals, *others):
    return lax.optimization_barrier((vals,) + others)[0]


class BlockSum:
    def __init__(self, to_peer, axis, n_dev):
        self.axis = axis
        self.n_dev = n_dev
        self.to_peer = to_peer.astype(BF16)
        self.from_peer = swap(self.to_peer, 1, n_dev)

    def cut(self, slot, half, vals=None):
        vals = self.own if vals is None else vals
        width = self.own.shape[self.axis] // 4
        middle = self.own.shape[1 - self.axis] // 2
        index = [None, None]
        index[self.axis] = slice(slot * width, (slot + 1) * width)
        index[1 - self.axis] = slice(half * middle, (half + 1) * middle)
        return vals[tuple(index)]

    plan = ((0, 2, 4, 1, 2), (1, 4, 2, 2, 1))

    def first(self, left, right):
        self.own = dot_f32(left, right, 0, 0) + self.from_peer.astype(F32)
        rounded = self.own.astype(BF16)
        self.came = []
        for half, first_bit, _, first_slot, _ in self.plan:
            sent = jnp.concatenate([self.cut(first_slot, half, rounded), self.cut(3, half, rounded)], axis=self.axis)
            self.came.append(swap(sent, first_bit, self.n_dev))
        return self.own

    def second(self):
        self.last = []
        self.near = []
        self.sent = []
        for came, (half, _, second_bit, _, second_slot) in zip(self.came, self.plan):
            near, far = jnp.split(came, 2, axis=self.axis)
            sent = (self.cut(second_slot, half) + far.astype(F32)).astype(BF16)
            self.sent.append(sent)
            self.near.append(near)
            self.last.append(swap(sent, second_bit, self.n_dev))
        return self.sent

    def total(self):
        self.last = lax.optimization_barrier(self.last)
        sums = []
        for half in range(2):
            sums.append(self.cut(0, half) + self.near[half].astype(F32) + self.last[half].astype(F32))
        return jnp.concatenate(sums, axis=1 - self.axis)


def solution(mesh):
    n_dev = mesh.shape['fsdp']

    def device_step(x_in, dy_out, ln_gain, w_q, w_k, w_v, w_o, w_gate, w_up, w_down):
        n_batch, seq_len, width = x_in.shape
        n_tok = n_batch * seq_len
        inner = w_q.shape[1]
        x2 = x_in.reshape(n_tok, width)
        dy2 = dy_out.reshape(n_tok, width)
        me = lax.axis_index('fsdp').astype(jnp.int32).reshape(1)

        def tp_peer(vals):
            return lax.ppermute(vals, 'tp', [(0, 1), (1, 0)])

        gain = lax.all_gather(ln_gain, 'fsdp', tiled=True).reshape(1, width)
        w_qkv = lax.all_gather(jnp.concatenate([w_q, w_k, w_v], axis=1), 'fsdp', axis=0, tiled=True)
        wo = lax.all_gather(w_o, 'fsdp', axis=1, tiled=True)
        wg = lax.all_gather(w_gate, 'fsdp', axis=0, tiled=True)
        wu = lax.all_gather(w_up, 'fsdp', axis=0, tiled=True)
        wd = lax.all_gather(w_down, 'fsdp', axis=1, tiled=True)

        half_dim = HEAD // 2
        inv_freq = jnp.power(10000.0, -2.0 * jnp.arange(half_dim, dtype=F32) / HEAD)
        angle = jnp.arange(seq_len, dtype=F32)[:, None] * inv_freq[None, :]
        cos_t = jnp.concatenate([jnp.cos(angle), jnp.cos(angle)], axis=1)
        sin_t = jnp.concatenate([-jnp.sin(angle), jnp.sin(angle)], axis=1)

        h_norm, h_own, h_peer, dy_own, dy_peer = prep(me, x2, dy2, gain)

        qkv = dot_f32(h_norm, w_qkv, 1, 0).astype(BF16)
        d_att = dot_f32(dy2, wo, 1, 1).astype(BF16)
        att, d_q, dkv = attention(qkv, d_att, cos_t, sin_t, seq_len)
        d_qkv = kv_finish(dkv, tp_peer(dkv), cos_t, sin_t, d_q)

        gate_val = dot_f32(h_norm, wg, 1, 0).astype(BF16)
        up_val = dot_f32(h_norm, wu, 1, 0).astype(BF16)
        act = swiglu(gate_val, up_val)

        def rows_of(vals, b):
            return vals[b * seq_len:(b + 1) * seq_len]

        def y_part(b, act_b):
            part = dot_f32(rows_of(att, b), wo, 1, 0) + dot_f32(rows_of(act_b, b), wd, 1, 0)
            part = part.astype(BF16)
            return part, tp_peer(part)

        column = lax.broadcasted_iota(jnp.int32, (1, inner + 2 * HEAD), 1)
        is_k = (column >= inner) & (column < inner + HEAD)
        is_v = column >= inner + HEAD
        skip = jnp.where(lax.axis_index('tp') == 0, is_v, is_k)
        w_back = jnp.where(skip, jnp.zeros((), BF16), w_qkv)

        def h_part(b, d_gate_b, d_up_b):
            part = dot_f32(rows_of(d_qkv, b), w_back, 1, 1) + dot_f32(rows_of(d_gate_b, b), wg, 1, 1)
            part = (part + dot_f32(rows_of(d_up_b, b), wu, 1, 1)).astype(BF16)
            return part, tp_peer(part)

        y0, y0_peer = y_part(0, act)
        y1, y1_peer = y_part(1, after(act, y0))
        down = BlockSum(dot_f32(after(act, y1), dy_peer, 0, 0), 1, n_dev)
        y2, y2_peer = y_part(2, after(act, down.to_peer))
        down_own = down.first(after(act, y2), dy_own)

        d_act = dot_f32(after(dy2, down_own), wd, 1, 1).astype(BF16)
        _, act_pull = jax.vjp(swiglu, gate_val, up_val)
        d_gate, d_up = act_pull(d_act)

        h0, h0_peer = h_part(0, d_gate, d_up)
        down_sent = down.second()
        gate = BlockSum(dot_f32(h_peer, after(d_gate, h0, *down_sent), 0, 0), 0, n_dev)
        h1, h1_peer = h_part(1, after(d_gate, gate.to_peer), d_up)
        gate_own = gate.first(h_own, after(d_gate, h1))
        y_out = y_finish(0, x2, after(y0, gate_own), y0_peer, None)
        y_out = y_finish(1, x2, after(y1, gate_own), y1_peer, y_out)
        up = BlockSum(dot_f32(h_peer, after(d_up, gate_own, y_out), 0, 0), 0, n_dev)
        h2, h2_peer = h_part(2, d_gate, after(d_up, up.to_peer))
        gate_sent = gate.second()
        up_own = up.first(h_own, after(d_up, h2, *gate_sent))
        grad_wdown = down.total()
        y_out = y_finish(2, x2, after(y2, up_own), y2_peer, y_out)

        att_late = after(att, up_own)
        small_o = BlockSum(dot_f32(att_late, dy_peer, 0, 0), 1, n_dev)
        d_late = after(d_qkv, small_o.to_peer)
        small_q = BlockSum(dot_f32(h_peer, d_late, 0, 0), 0, n_dev)
        o_own = small_o.first(after(att_late, small_q.to_peer), dy_own)
        q_own = small_q.first(h_own, after(d_late, o_own))
        grad_wgate = gate.total()
        up_sent = up.second()
        grad_x, gain_part = norm_finish(0, x2, dy2, after(h0, q_own, *up_sent), h0_peer, gain, None)
        o_sent = small_o.second()
        q_sent = small_q.second()
        grad_x, gain_b = norm_finish(1, x2, dy2, after(h1, q_own, *up_sent), h1_peer, gain, grad_x)
        gain_part = gain_part + gain_b
        grad_wup = up.total()
        grad_wo = small_o.total()
        grad_qkv = small_q.total()
        grad_x, gain_b = norm_finish(2, x2, dy2, after(h2, *o_sent, *q_sent), h2_peer, gain, grad_x)
        gain_part = gain_part + gain_b
        grad_gain = lax.psum_scatter(gain_part.reshape(width), 'fsdp', scatter_dimension=0, tiled=True)

        shape = (n_batch, seq_len, width)
        return (y_out.reshape(shape), grad_x.reshape(shape), grad_gain, grad_qkv[:, :inner], grad_qkv[:, inner:inner + HEAD], grad_qkv[:, inner + HEAD:], grad_wo, grad_wgate, grad_wup, grad_wdown)

    act_spec = P('fsdp', None, None)
    row_spec = P('fsdp', 'tp')
    kv_spec = P('fsdp', None)
    col_spec = P('tp', 'fsdp')
    in_specs = (act_spec, act_spec, P('fsdp'), row_spec, kv_spec, kv_spec, col_spec, row_spec, row_spec, col_spec)
    out_specs = (act_spec, act_spec, P('fsdp'), row_spec, kv_spec, kv_spec, col_spec, row_spec, row_spec, col_spec)

    return jax.shard_map(device_step, mesh=mesh, in_specs=in_specs, out_specs=out_specs, check_vma=False)
```
